256 devices in a mesh: lat: 8 (over x_lo, y), lon: 32 (over z, x_hi, core).
Axes of the slice: x: 4 (x_hi: 2, x_lo: 2; x = x_hi * 2 + x_lo), y: 4, z: 8, core: 2. Of those that a mesh axis runs over, the one named last changes fastest.
Arguments:
- field: bfloat16 [256, 1024, 512], P('lat', 'lon'), may hold values from -6 to 6
- qkv_fine: bfloat16 [512, 1536], replicated, may hold values from -0.35355339 to 0.35355339
- proj_fine: bfloat16 [512, 512], replicated, may hold values from -0.25 to 0.25
- up_fine: bfloat16 [512, 2048], replicated, may hold values from -0.25 to 0.25
- down_fine: bfloat16 [2048, 512], replicated, may hold values from -0.125 to 0.125
- merge_weight: bfloat16 [2048, 1024], replicated, may hold values from -0.15467961 to 0.15467961
- qkv_coarse: bfloat16 [1024, 3072], P(None, 'lon'), may hold values from -0.25 to 0.25
- proj_coarse: bfloat16 [1024, 1024], P(None, 'lon'), may hold values from -0.1875 to 0.1875
Outputs:
- fine_out: bfloat16 [256, 1024, 512], P('lat', 'lon')
- coarse_out: bfloat16 [128, 512, 1024], P('lat', 'lon')
The draws below stay inside these ranges and needn't reach their ends.
All inputs are finite; a program needn't handle non-finite values.
Results may differ from the reference program's by a relative error of at most 0.018.
Values may be sent and summed in bfloat16 or wider, within the bound.
A program may use at most 128 MiB of HBM per device.

```python
import jax
import jax.numpy as jnp
from jax import lax

C1 = 512
C2 = 1024
HID1 = 2048
HEAD = 64
WIN = 16
H1 = 256
W1 = 1024


def draw_field(key, part):
    noise_key = jax.random.fold_in(jax.random.fold_in(key, 101), 0)
    noise = jnp.clip(jax.random.normal(noise_key, (H1, W1, C1), jnp.float32), -6.0, 6.0)
    return noise.astype(jnp.bfloat16)


def draw_qkv_fine(key, part):
    base = jnp.clip(jax.random.normal(jax.random.fold_in(key, 202), (C1, 3 * C1), jnp.float32), -6.0, 6.0)
    base = base * C1 ** (-0.5)
    return base.astype(jnp.bfloat16)


def draw_merge_weight(key, part):
    base = jnp.clip(jax.random.normal(jax.random.fold_in(key, 303), (4 * C1, C2), jnp.float32), -6.0, 6.0)
    base = base * (4 * C1) ** (-0.5)
    return base.astype(jnp.bfloat16)


def draw_qkv_coarse(key, part):
    base = jnp.clip(jax.random.normal(jax.random.fold_in(key, 404), (C2, 3 * C2), jnp.float32), -6.0, 6.0)
    base = base * C2 ** (-0.5)
    return base.astype(jnp.bfloat16)


def steps_of(own_key, shape, cuts, least, largest):
    def one(axis_at, parts):
        steps = jax.random.uniform(jax.random.fold_in(jax.random.fold_in(own_key, 6), axis_at), (parts,), jnp.float32, least / len(cuts), largest / len(cuts))
        return jnp.repeat(jnp.exp(steps), shape[axis_at] // parts).reshape((-1,) + (1,) * (len(shape) - axis_at - 1))

    loudness = one(*cuts[0])
    for cut in cuts[1:]:
        loudness = loudness * one(*cut)
    return loudness


def centred(rng, shape, scale, most, shards=(), kind=jnp.bfloat16):
    values = jax.random.normal(rng, shape, jnp.float32) * scale
    if len(shards) > 0:
        values = steps_of(rng, shape, shards, -0.22, 0.18) * values
    return jnp.clip(values, min=-most, max=most).astype(kind)


def setup_inputs(seed: int = 0) -> dict:
    key_of = jax.random.split(jax.random.key(seed), 9)
    field = draw_field(jax.random.fold_in(key_of[8], 71), 0)
    qkv_fine = draw_qkv_fine(jax.random.fold_in(key_of[8], 71), 0)
    proj_fine = centred(key_of[2], (C1, C1), C1 ** -0.5, 0.25)
    up_fine = centred(key_of[3], (C1, HID1), C1 ** -0.5, 0.25)
    down_fine = centred(key_of[4], (HID1, C1), HID1 ** -0.5, 0.125)
    merge_weight = draw_merge_weight(jax.random.fold_in(key_of[8], 71), 0)
    qkv_coarse = draw_qkv_coarse(jax.random.fold_in(key_of[8], 71), 0)
    proj_coarse = centred(key_of[7], (C2, C2), C2 ** -0.5, 0.1875, ((1, 32),))
    return dict(field=field, qkv_fine=qkv_fine, proj_fine=proj_fine, up_fine=up_fine, down_fine=down_fine, merge_weight=merge_weight, qkv_coarse=qkv_coarse, proj_coarse=proj_coarse)


def normalize(values):
    values = values.astype(jnp.float32)
    center = values - lax.optimization_barrier(jnp.mean(values, axis=-1, keepdims=True))
    spread = lax.optimization_barrier(jnp.mean(center * center, axis=-1, keepdims=True))
    return center * lax.rsqrt(spread + 1e-05)

def window_core(qkv, label):
    cols_total = qkv.shape[1]
    width = qkv.shape[2] // 3
    heads = width // HEAD
    blocks = cols_total // WIN
    packed = qkv.reshape(WIN, blocks, WIN, 3, heads, HEAD).transpose(3, 1, 4, 0, 2, 5)
    packed = packed.reshape(3, blocks, heads, WIN * WIN, HEAD).astype(jnp.float32)
    scores = jnp.einsum('nhqd,nhkd->nhqk', packed[0], packed[1]) * HEAD ** (-0.5)
    tags = jnp.repeat(label, WIN)
    allowed = tags[:, None] == tags[None, :]
    scores = jnp.where(allowed, scores, -1e+30)
    weights = jax.nn.softmax(scores, axis=-1).astype(jnp.bfloat16)
    mixed = jnp.einsum('nhqk,nhkd->nhqd', weights.astype(jnp.float32), packed[2]).astype(jnp.bfloat16)
    mixed = mixed.reshape(blocks, heads, WIN, WIN, HEAD).transpose(2, 0, 3, 1, 4)
    return mixed.reshape(WIN, cols_total, width)

def shifted_mix(values, w_qkv):
    rows_total, cols_total, width = values.shape
    half_win = WIN // 2
    rolled = jnp.roll(values, (-half_win, -half_win), (0, 1))
    anchor = (jnp.arange(rows_total, dtype=jnp.int32) + half_win) % rows_total
    label = (anchor < half_win).astype(jnp.int32).reshape(rows_total // WIN, WIN)

    def one_strip(pair):
        strip, tags = pair
        normed = normalize(strip).astype(jnp.bfloat16).reshape(-1, width)
        qkv = jnp.dot(normed, w_qkv, preferred_element_type=jnp.float32).astype(jnp.bfloat16)
        return window_core(qkv.reshape(WIN, cols_total, 3 * width), tags)
    mixed = lax.map(one_strip, (rolled.reshape(rows_total // WIN, WIN, cols_total, width), label))
    mixed = mixed.reshape(rows_total, cols_total, width)
    return jnp.roll(mixed, (half_win, half_win), (0, 1))

def reference(field, qkv_fine, proj_fine, up_fine, down_fine, merge_weight, qkv_coarse, proj_coarse):
    rows_total, cols_total, width = field.shape
    mixed = shifted_mix(field, qkv_fine)

    def finish(pair):
        strip, part = pair
        attend = jnp.dot(part.reshape(-1, width), proj_fine, preferred_element_type=jnp.float32)
        attended = (strip.reshape(-1, width).astype(jnp.float32) + attend).astype(jnp.bfloat16)
        normed = normalize(attended).astype(jnp.bfloat16)
        hidden = jax.nn.gelu(jnp.dot(normed, up_fine, preferred_element_type=jnp.float32)).astype(jnp.bfloat16)
        output = attended.astype(jnp.float32) + jnp.dot(hidden, down_fine, preferred_element_type=jnp.float32)
        return output.astype(jnp.bfloat16).reshape(WIN, cols_total, width)
    strips = rows_total // WIN
    fine_out = lax.map(finish, (field.reshape(strips, WIN, cols_total, width), mixed.reshape(strips, WIN, cols_total, width)))
    fine_out = fine_out.reshape(rows_total, cols_total, width)
    joined = fine_out.reshape(rows_total // 2, 2, cols_total // 2, 2, width).transpose(0, 2, 3, 1, 4)
    joined = joined.reshape(-1, 4 * width)
    merged = jnp.dot(normalize(joined).astype(jnp.bfloat16), merge_weight, preferred_element_type=jnp.float32)
    wide = merge_weight.shape[1]
    merged = merged.astype(jnp.bfloat16).reshape(rows_total // 2, cols_total // 2, wide)
    coarse_mix = shifted_mix(merged, qkv_coarse)
    attend = jnp.dot(coarse_mix.reshape(-1, wide), proj_coarse, preferred_element_type=jnp.float32)
    coarse_out = (merged.reshape(-1, wide).astype(jnp.float32) + attend).astype(jnp.bfloat16)
    return (fine_out, coarse_out.reshape(rows_total // 2, cols_total // 2, wide))
```

```python
import jax
import jax.numpy as jnp
from jax import lax
from jax.experimental import pallas as pl
from jax.experimental.pallas import tpu as pltpu
from jax.sharding import PartitionSpec as P

MESH = pl.DeviceIdType.MESH
BF = jnp.bfloat16
F32 = jnp.float32
OFFSETS = (0, -1, 1, -2, 2, -3, 3, 4)
CHUNKS = ((0, 1), (1, 2), (3, 2), (5, 2), (7, 1))


def norm(v):
    center = v - jnp.mean(v, axis=-1, keepdims=True)
    spread = jnp.mean(center * center, axis=-1, keepdims=True)
    return center * lax.rsqrt(spread + 1e-05)


def dot(a, b):
    return jnp.dot(a, b, preferred_element_type=F32)


def attend_pair(keys, qt, vt, bias):
    zero = jnp.zeros((64, 256), BF)
    outs = []
    for half in range(2):
        part = qt[64 * half : 64 * half + 64]
        padded = jnp.concatenate([part, zero] if half == 0 else [zero, part], axis=0)
        scores = dot(keys, padded) + bias
        top = jnp.max(scores, axis=0, keepdims=True)
        p = jnp.exp(scores - top)
        total = jnp.sum(p, axis=0, keepdims=True)
        o = dot(vt[64 * half : 64 * half + 64], p.astype(BF))
        outs.append(o * (1.0 / total))
    return jnp.concatenate(outs, axis=0)


def kernel(
    field, wqkv_h, wproj_h, wup_h, wdown_h, wmerge_h, wsh,
    fine_out, coarse_out,
    wqkv, wproj, wup, wdown, wmerge,
    fv, xr, mr, mo, fo, fs, jn, mg, cr, cxt, wall, qkvt, ot, cm, cmo, co, pt,
    lsem, osem, hs, hr, bs, br, cs, cq, ds_, dr, zs, zr, xs, xq, ps, pr, es, er, gs, gr,
):
    lat = lax.axis_index("lat")
    lon = lax.axis_index("lon")
    xlo = lat // 4
    y = lat % 4
    z = lon // 4
    xh = (lon // 2) % 2
    c = lon % 2
    west = (lat, (lon + 31) % 32)
    east = (lat, (lon + 1) % 32)
    north = ((lat + 7) % 8, lon)
    south = ((lat + 1) % 8, lon)
    northwest = ((lat + 7) % 8, (lon + 31) % 32)
    southeast = ((lat + 1) % 8, (lon + 1) % 32)
    zup = (lat, ((z + 1) % 8) * 4 + xh * 2 + c)
    zdn = (lat, ((z + 7) % 8) * 4 + xh * 2 + c)
    cross = ((1 - xlo) * 4 + y, z * 4 + (1 - xh) * 2 + c)
    pair = ((1 - xlo) * 4 + y, lon)
    twin = (lat, z * 4 + xh * 2 + (1 - c))

    def local(src, dst, at):
        copy = pltpu.make_async_copy(src, dst, lsem.at[at])
        copy.start()
        return copy

    sent = []

    def remote(src, dst, ssem, rsem, at, device):
        copy = pltpu.make_async_remote_copy(
            src_ref=src, dst_ref=dst, send_sem=ssem.at[at], recv_sem=rsem.at[at],
            device_id=device, device_id_type=MESH,
        )
        copy.start()
        sent.append(copy)
        return copy

    own_x = local(field.at[pl.ds(8, 24), pl.ds(1, 3)], xr.at[pl.ds(0, 24), pl.ds(0, 3)], 0)
    l_qkv = local(wqkv_h, wqkv, 1)
    own_w = local(wsh, wall.at[xh, c, 0], 7)
    own_f = local(field, fv, 2)
    l_proj = local(wproj_h, wproj, 3)
    l_up = local(wup_h, wup, 4)
    l_down = local(wdown_h, wdown, 5)
    l_merge = local(wmerge_h, wmerge, 6)

    barrier = pltpu.get_barrier_semaphore()
    peers = (west, east, north, south, northwest, southeast, zup, zdn, cross, pair, twin)
    for peer in peers:
        pl.semaphore_signal(barrier, inc=1, device_id=peer, device_id_type=MESH)
    pl.semaphore_wait(barrier, len(peers))

    h = [
        remote(field.at[pl.ds(8, 24), 0], xr.at[pl.ds(0, 24), 3], hs, hr, 0, west),
        remote(field.at[pl.ds(0, 8), pl.ds(1, 3)], xr.at[pl.ds(24, 8), pl.ds(0, 3)], hs, hr, 1, north),
        remote(field.at[pl.ds(0, 8), 0], xr.at[pl.ds(24, 8), 3], hs, hr, 2, northwest),
    ]

    zc, xc, pc, ec, gc = {}, {}, {}, {}, {}

    def send_z(step):
        if step == 0:
            zc[0] = remote(wsh, wall.at[xh, c, 1], zs, zr, 0, zup)
            zc[1] = remote(wsh, wall.at[xh, c, 2], zs, zr, 1, zdn)
        elif step < 3:
            a = 2 * step
            zc[a] = remote(wall.at[xh, c, a - 1], wall.at[xh, c, a + 1], zs, zr, a, zup)
            zc[a + 1] = remote(wall.at[xh, c, a], wall.at[xh, c, a + 2], zs, zr, a + 1, zdn)
        else:
            zc[6] = remote(wall.at[xh, c, 5, 0], wall.at[xh, c, 7, 0], zs, zr, 6, zup)
            zc[7] = remote(wall.at[xh, c, 6, 1], wall.at[xh, c, 7, 1], zs, zr, 7, zdn)

    def own_chunk(k):
        at, n = CHUNKS[k]
        if k == 0:
            src_half, src = wsh.at[xlo], wsh
            dst_half, dst = wall.at[xh, c, 0, xlo], wall.at[xh, c, 0]
        else:
            src_half = dst_half = wall.at[xh, c, pl.ds(at, n), xlo]
            src = dst = wall.at[xh, c, pl.ds(at, n)]
        xc[k] = remote(src_half, dst_half, xs, xq, k, cross)
        ec[k] = remote(src, dst, es, er, k, twin)

    def pass_cross(k):
        at, n = CHUNKS[k]
        xc[k].wait_recv()
        ref = wall.at[1 - xh, c, pl.ds(at, n), 1 - xlo]
        pc[k] = remote(ref, ref, ps, pr, k, pair)

    def pass_twin(k):
        at, n = CHUNKS[k]
        pc[k].wait_recv()
        ref = wall.at[1 - xh, c, pl.ds(at, n)]
        gc[k] = remote(ref, ref, gs, gr, k, twin)

    send_z(0)
    own_chunk(0)

    def forward(k):
        zc[2 * k - 2].wait_recv()
        zc[2 * k - 1].wait_recv()
        if k < 4:
            send_z(k)
        own_chunk(k)
        pass_cross(k - 1)
        if k >= 2:
            pass_twin(k - 2)

    off_half = (lax.broadcasted_iota(jnp.int32, (256, 256), 0) >= 128) != (
        lax.broadcasted_iota(jnp.int32, (256, 256), 1) >= 128
    )
    edge = lat == 7

    def fine_window(wr, wc):
        lift = jnp.where(jnp.logical_and(edge, wr == 1), F32(-1e30), F32(0.0))
        bias = jnp.where(off_half, lift, F32(0.0))
        x = xr[pl.ds(16 * wr, 16), pl.ds(2 * wc, 2)].astype(F32).reshape(256, 512)
        xn = norm(x).astype(BF)
        q = (dot(xn, wqkv[:, 0:512])).astype(BF).astype(F32) * 0.125
        keys = dot(xn, wqkv[:, 512:1024]).astype(BF)
        v = dot(xn, wqkv[:, 1024:1536])
        qt = q.T.astype(BF)
        vt = v.T.astype(BF)
        outs = []
        for j in range(4):
            cut = slice(128 * j, 128 * j + 128)
            outs.append(attend_pair(keys[:, cut], qt[cut], vt[cut], bias).T)
        res = jnp.concatenate(outs, axis=1)
        mr[pl.ds(16 * wr, 16), pl.ds(2 * wc, 2)] = res.reshape(16, 2, 8, 512).astype(BF)

    own_x.wait()
    l_qkv.wait()
    own_w.wait()
    fine_window(0, 0)
    for copy in h:
        copy.wait_recv()

    b = [None] * 5

    @pl.loop(0, 3)
    def _(step):
        wr = jnp.where(step == 1, 0, 1)
        wc = jnp.where(step == 2, 0, 1)
        fine_window(wr, wc)

    forward(1)
    b[0] = remote(mr.at[pl.ds(0, 24), 3], mo.at[pl.ds(8, 24), 0], bs, br, 0, east)
    b[1] = remote(mr.at[pl.ds(24, 8), pl.ds(0, 3)], mo.at[pl.ds(0, 8), pl.ds(1, 3)], bs, br, 1, south)
    b[2] = remote(mr.at[pl.ds(24, 8), 3], mo.at[pl.ds(0, 8), 0], bs, br, 2, southeast)
    mo[pl.ds(8, 24), pl.ds(1, 3)] = mr[pl.ds(0, 24), pl.ds(0, 3)]
    for copy in (own_f, l_proj, l_up, l_down, l_merge):
        copy.wait()
    for copy in b[:3]:
        copy.wait_recv()

    def fine_chunk(k):
        rows = pl.ds(8 * k, 8)
        x = fv[rows].astype(F32).reshape(256, 512)
        mx = mo[rows].astype(F32).reshape(256, 512).astype(BF)
        att = (x + dot(mx, wproj[...])).astype(BF).astype(F32)
        n = norm(att).astype(BF)
        acc = att
        for s in range(4):
            cut = slice(512 * s, 512 * s + 512)
            hid = jax.nn.gelu(dot(n, wup[:, cut])).astype(BF)
            acc = acc + dot(hid, wdown[cut, :])
        out = acc.astype(BF)
        out32 = out.astype(F32)
        fo[rows] = out32.reshape(8, 4, 8, 512).astype(BF)
        for t in range(4):
            fs[t] = out32[:, 128 * t : 128 * t + 128]
        for i in range(4):
            joined = jnp.concatenate(
                [
                    fs[t, pl.ds(64 * i + 32 * (p % 2) + p // 2, 16, stride=2), :]
                    for p in range(4)
                    for t in range(4)
                ],
                axis=1,
            )
            jn[pl.ds(pl.multiple_of(64 * k + 16 * i, 16), 16), :] = norm(joined).astype(BF)

    @pl.loop(0, 2)
    def _(k):
        fine_chunk(k)

    forward(2)

    @pl.loop(2, 4)
    def _(k):
        fine_chunk(k)

    forward(3)
    out_f = pltpu.make_async_copy(fo, fine_out, osem.at[0])
    out_f.start()

    @pl.loop(0, 4)
    def _(s):
        cut = pl.ds(pl.multiple_of(256 * s, 256), 256)
        m = dot(jn[...], wmerge[:, cut])
        mg[:, :, :, cut] = m.reshape(16, 2, 8, 256).astype(BF)

    a = [
        remote(mg.at[pl.ds(8, 8), 0], cr.at[pl.ds(0, 8), 1], cs, cq, 0, west),
        remote(mg.at[pl.ds(0, 8), 1], cr.at[pl.ds(8, 8), 0], cs, cq, 1, north),
        remote(mg.at[pl.ds(0, 8), 0], cr.at[pl.ds(8, 8), 1], cs, cq, 2, northwest),
    ]
    cr[pl.ds(0, 8), 0] = mg[pl.ds(8, 8), 1]
    forward(4)
    for copy in a:
        copy.wait_recv()
    cxt[...] = norm(cr[...].astype(F32).reshape(256, 1024)).T.astype(BF)
    pass_cross(4)
    pass_twin(3)
    pass_twin(4)
    for k in range(5):
        ec[k].wait_recv()
    for k in range(5):
        gc[k].wait_recv()

    @pl.loop(0, 4)
    def _(g):
        for r2 in range(2):
            w = wall[g // 2, g % 2, pl.ds(4 * r2, 4)].reshape(512, 1024)
            got = dot(w, cxt[...]).astype(BF)
            for i in range(4):
                slot = ((z + OFFSETS[4 * r2 + i] + 8) % 8) * 4 + g
                at = pl.multiple_of(96 * slot, 32)
                qkvt[pl.ds(at, 96), :] = got[128 * i : 128 * i + 96]
                pt[pl.ds(pl.multiple_of(32 * slot, 32), 32), :] = wall[
                    g // 2, g % 2, 4 * r2 + i, 1, pl.ds(32, 32), :
                ]

    c_lift = jnp.where(edge, F32(-1e30), F32(0.0))

    @pl.loop(0, 8)
    def _(j):
        bias = jnp.where(off_half, c_lift, F32(0.0))
        at = pl.multiple_of(128 * j, 128)
        qt = (qkvt[pl.ds(at, 128), :].astype(F32) * 0.125).astype(BF)
        keys = qkvt[pl.ds(at + 1024, 128), :].astype(F32).T.astype(BF)
        vt = qkvt[pl.ds(at + 2048, 128), :]
        o = attend_pair(keys, qt, vt, bias).T
        cm[:, :, :, pl.ds(at, 128)] = o.reshape(16, 2, 8, 128).astype(BF)

    d = [
        remote(cm.at[pl.ds(0, 8), 1], cmo.at[pl.ds(8, 8), 0], ds_, dr, 0, east),
        remote(cm.at[pl.ds(8, 8), 0], cmo.at[pl.ds(0, 8), 1], ds_, dr, 1, south),
        remote(cm.at[pl.ds(8, 8), 1], cmo.at[pl.ds(0, 8), 0], ds_, dr, 2, southeast),
    ]
    cmo[pl.ds(8, 8), 1] = cm[pl.ds(0, 8), 0]
    for copy in d:
        copy.wait_recv()
    mixed = cmo[...].astype(F32).reshape(256, 1024).astype(BF)
    ot[...] = mixed

    @pl.loop(0, 4)
    def _(s):
        at = pl.multiple_of(256 * s, 256)
        got = lax.dot_general(
            ot[...], pt[pl.ds(at, 256), :], (((1,), (1,)), ((), ())), preferred_element_type=F32
        )
        cut = pl.ds(at, 256)
        res = mg[:, :, :, cut].astype(F32) + got.reshape(16, 2, 8, 256)
        co[:, :, :, cut] = res.astype(BF)

    out_c = pltpu.make_async_copy(co, coarse_out, osem.at[1])
    out_c.start()
    for copy in sent:
        copy.wait_send()
    out_f.wait()
    out_c.wait()


def body(field, qkv_fine, proj_fine, up_fine, down_fine, merge_weight, qkv_coarse, proj_coarse):
    shard = jnp.concatenate([qkv_coarse.T, proj_coarse.T], axis=0).reshape(2, 64, 1024)
    any_spec = pl.BlockSpec(memory_space=pl.ANY)
    dma = pltpu.SemaphoreType.DMA
    vm = pltpu.VMEM
    fine, coarse = pl.pallas_call(
        kernel,
        out_shape=(
            jax.ShapeDtypeStruct((32, 4, 8, 512), BF),
            jax.ShapeDtypeStruct((16, 2, 8, 1024), BF),
        ),
        in_specs=[any_spec] * 7,
        out_specs=(any_spec, any_spec),
        scratch_shapes=[
            vm((512, 1536), BF), vm((512, 512), BF), vm((512, 2048), BF), vm((2048, 512), BF),
            vm((2048, 1024), BF),
            vm((32, 4, 8, 512), BF), vm((32, 4, 8, 512), BF), vm((32, 4, 8, 512), BF),
            vm((32, 4, 8, 512), BF), vm((32, 4, 8, 512), BF),
            vm((4, 256, 128), F32), vm((256, 2048), BF),
            vm((16, 2, 8, 1024), BF), vm((16, 2, 8, 1024), BF), vm((1024, 256), BF),
            vm((2, 2, 8, 2, 64, 1024), BF), vm((3072, 256), BF), vm((256, 1024), BF),
            vm((16, 2, 8, 1024), BF), vm((16, 2, 8, 1024), BF), vm((16, 2, 8, 1024), BF),
            vm((1024, 1024), BF),
            dma((8,)), dma((2,)),
            dma((3,)), dma((3,)), dma((3,)), dma((3,)), dma((3,)), dma((3,)), dma((3,)), dma((3,)),
            dma((8,)), dma((8,)), dma((5,)), dma((5,)), dma((5,)), dma((5,)),
            dma((5,)), dma((5,)), dma((5,)), dma((5,)),
        ],
        compiler_params=pltpu.CompilerParams(
            collective_id=0, has_side_effects=True, vmem_limit_bytes=60 * 1024 * 1024
        ),
        name="encoder",
    )(field.reshape(32, 4, 8, 512), qkv_fine, proj_fine, up_fine, down_fine, merge_weight, shard)
    return fine.reshape(32, 32, 512), coarse.reshape(16, 16, 1024)


def solution(mesh):
    in_specs = (P("lat", "lon", None), P(), P(), P(), P(), P(), P(None, "lon"), P(None, "lon"))
    out_specs = (P("lat", "lon", None), P("lat", "lon", None))
    return jax.shard_map(body, mesh=mesh, in_specs=in_specs, out_specs=out_specs, check_vma=False)
```

```python
import jax
import jax.numpy as jnp
from jax import lax
from jax.experimental import pallas as pl
from jax.experimental.pallas import tpu as pltpu
from jax.sharding import PartitionSpec as P

MESH = pl.DeviceIdType.MESH
BF = jnp.bfloat16
F32 = jnp.float32
OFFSETS = (0, -1, 1, -2, 2, -3, 3, 4)
CHUNKS = ((0, 1), (1, 2), (3, 2), (5, 2), (7, 1))


def norm(v):
    center = v - jnp.mean(v, axis=-1, keepdims=True)
    spread = jnp.mean(center * center, axis=-1, keepdims=True)
    return center * lax.rsqrt(spread + 1e-05)


def dot(a, b):
    return jnp.dot(a, b, preferred_element_type=F32)


def attend_pair(keys, qt, vt, bias):
    zero = jnp.zeros((64, 256), BF)
    outs = []
    for half in range(2):
        part = qt[64 * half : 64 * half + 64]
        padded = jnp.concatenate([part, zero] if half == 0 else [zero, part], axis=0)
        scores = dot(keys, padded) + bias
        top = jnp.max(scores, axis=0, keepdims=True)
        p = jnp.exp(scores - top)
        total = jnp.sum(p, axis=0, keepdims=True)
        o = dot(vt[64 * half : 64 * half + 64], p.astype(BF))
        outs.append(o * (1.0 / total))
    return jnp.concatenate(outs, axis=0)


def kernel(
    field, wqkv_h, wproj_h, wup_h, wdown_h, wmerge_h, cqkv_h, cproj_h,
    fine_out, coarse_out,
    wqkv, wproj, wup, wdown, wmerge, cqkv, cproj,
    fv, xr, mr, mo, fo, fs, jn, mg, cr, cxt, wall, qkvt, ot, cm, cmo, co, pt,
    lsem, osem, hs, hr, bs, br, cs, cq, ds_, dr, zs, zr, xs, xq, ps, pr, es, er, gs, gr,
):
    lat = lax.axis_index("lat")
    lon = lax.axis_index("lon")
    xlo = lat // 4
    y = lat % 4
    z = lon // 4
    xh = (lon // 2) % 2
    c = lon % 2
    west = (lat, (lon + 31) % 32)
    east = (lat, (lon + 1) % 32)
    north = ((lat + 7) % 8, lon)
    south = ((lat + 1) % 8, lon)
    northwest = ((lat + 7) % 8, (lon + 31) % 32)
    southeast = ((lat + 1) % 8, (lon + 1) % 32)
    zup = (lat, ((z + 1) % 8) * 4 + xh * 2 + c)
    zdn = (lat, ((z + 7) % 8) * 4 + xh * 2 + c)
    cross = ((1 - xlo) * 4 + y, z * 4 + (1 - xh) * 2 + c)
    pair = ((1 - xlo) * 4 + y, lon)
    twin = (lat, z * 4 + xh * 2 + (1 - c))

    def local(src, dst, at):
        copy = pltpu.make_async_copy(src, dst, lsem.at[at])
        copy.start()
        return copy

    sent = []

    def remote(src, dst, ssem, rsem, at, device):
        copy = pltpu.make_async_remote_copy(
            src_ref=src, dst_ref=dst, send_sem=ssem.at[at], recv_sem=rsem.at[at],
            device_id=device, device_id_type=MESH,
        )
        copy.start()
        sent.append(copy)
        return copy

    own_x = local(field.at[pl.ds(8, 24), pl.ds(1, 3)], xr.at[pl.ds(0, 24), pl.ds(0, 3)], 0)
    own_q = local(cqkv_h, cqkv, 7)
    own_p = local(cproj_h, cproj, 8)
    l_qkv = local(wqkv_h, wqkv, 1)
    own_f = local(field, fv, 2)
    l_proj = local(wproj_h, wproj, 3)
    l_up = local(wup_h, wup, 4)
    l_down = local(wdown_h, wdown, 5)
    l_merge = local(wmerge_h, wmerge, 6)

    barrier = pltpu.get_barrier_semaphore()
    peers = (west, east, north, south, northwest, southeast, zup, zdn, cross, pair, twin)
    for peer in peers:
        pl.semaphore_signal(barrier, inc=1, device_id=peer, device_id_type=MESH)
    pl.semaphore_wait(barrier, len(peers))

    h = [
        remote(field.at[pl.ds(8, 24), 0], xr.at[pl.ds(0, 24), 3], hs, hr, 0, west),
        remote(field.at[pl.ds(0, 8), pl.ds(1, 3)], xr.at[pl.ds(24, 8), pl.ds(0, 3)], hs, hr, 1, north),
        remote(field.at[pl.ds(0, 8), 0], xr.at[pl.ds(24, 8), 3], hs, hr, 2, northwest),
    ]

    zc, xc, pc, ec, gc = {}, {}, {}, {}, {}

    def send_z(step):
        if step == 0:
            zc[0] = remote(wall.at[xh, c, 0], wall.at[xh, c, 1], zs, zr, 0, zup)
            zc[1] = remote(wall.at[xh, c, 0], wall.at[xh, c, 2], zs, zr, 1, zdn)
        elif step < 3:
            a = 2 * step
            zc[a] = remote(wall.at[xh, c, a - 1], wall.at[xh, c, a + 1], zs, zr, a, zup)
            zc[a + 1] = remote(wall.at[xh, c, a], wall.at[xh, c, a + 2], zs, zr, a + 1, zdn)
        else:
            zc[6] = remote(wall.at[xh, c, 5, 0], wall.at[xh, c, 7, 0], zs, zr, 6, zup)
            zc[7] = remote(wall.at[xh, c, 6, 1], wall.at[xh, c, 7, 1], zs, zr, 7, zdn)

    def own_chunk(k):
        at, n = CHUNKS[k]
        half = wall.at[xh, c, pl.ds(at, n), xlo]
        full = wall.at[xh, c, pl.ds(at, n)]
        xc[k] = remote(half, half, xs, xq, k, cross)
        ec[k] = remote(full, full, es, er, k, twin)

    def pass_cross(k):
        at, n = CHUNKS[k]
        xc[k].wait_recv()
        ref = wall.at[1 - xh, c, pl.ds(at, n), 1 - xlo]
        pc[k] = remote(ref, ref, ps, pr, k, pair)

    def pass_twin(k):
        at, n = CHUNKS[k]
        pc[k].wait_recv()
        ref = wall.at[1 - xh, c, pl.ds(at, n)]
        gc[k] = remote(ref, ref, gs, gr, k, twin)

    own_q.wait()
    own_p.wait()
    for t in range(4):
        rows = slice(256 * t, 256 * t + 256)
        shard = jnp.concatenate([cqkv[rows, :].astype(F32), cproj[rows, :].astype(F32)], axis=1)
        wall[xh, c, 0, :, :, rows] = shard.T.astype(BF).reshape(2, 64, 256)
    send_z(0)
    own_chunk(0)

    def forward(k):
        zc[2 * k - 2].wait_recv()
        zc[2 * k - 1].wait_recv()
        if k < 4:
            send_z(k)
        own_chunk(k)
        pass_cross(k - 1)
        if k >= 2:
            pass_twin(k - 2)

    off_half = (lax.broadcasted_iota(jnp.int32, (256, 256), 0) >= 128) != (
        lax.broadcasted_iota(jnp.int32, (256, 256), 1) >= 128
    )
    edge = lat == 7

    def fine_window(wr, wc):
        lift = jnp.where(jnp.logical_and(edge, wr == 1), F32(-1e30), F32(0.0))
        bias = jnp.where(off_half, lift, F32(0.0))
        x = xr[pl.ds(16 * wr, 16), pl.ds(2 * wc, 2)].astype(F32).reshape(256, 512)
        xn = norm(x).astype(BF)
        q = (dot(xn, wqkv[:, 0:512])).astype(BF).astype(F32) * 0.125
        keys = dot(xn, wqkv[:, 512:1024]).astype(BF)
        v = dot(xn, wqkv[:, 1024:1536])
        qt = q.T.astype(BF)
        vt = v.T.astype(BF)
        outs = []
        for j in range(4):
            cut = slice(128 * j, 128 * j + 128)
            outs.append(attend_pair(keys[:, cut], qt[cut], vt[cut], bias).T)
        res = jnp.concatenate(outs, axis=1)
        mr[pl.ds(16 * wr, 16), pl.ds(2 * wc, 2)] = res.reshape(16, 2, 8, 512).astype(BF)

    own_x.wait()
    l_qkv.wait()
    fine_window(0, 0)
    h[0].wait_recv()
    fine_window(0, 1)
    b = [remote(mr.at[pl.ds(0, 16), 3], mo.at[pl.ds(8, 16), 0], bs, br, 0, east)]
    h[1].wait_recv()
    h[2].wait_recv()
    forward(1)
    fine_window(1, 0)
    b.append(remote(mr.at[pl.ds(24, 8), pl.ds(0, 2)], mo.at[pl.ds(0, 8), pl.ds(1, 2)], bs, br, 1, south))
    fine_window(1, 1)
    b.append(remote(mr.at[pl.ds(16, 8), 3], mo.at[pl.ds(24, 8), 0], bs, br, 2, east))
    b.append(remote(mr.at[pl.ds(24, 8), 2], mo.at[pl.ds(0, 8), 3], bs, br, 3, south))
    b.append(remote(mr.at[pl.ds(24, 8), 3], mo.at[pl.ds(0, 8), 0], bs, br, 4, southeast))
    forward(2)
    mo[pl.ds(8, 24), pl.ds(1, 3)] = mr[pl.ds(0, 24), pl.ds(0, 3)]
    for copy in (own_f, l_proj, l_up, l_down, l_merge):
        copy.wait()

    def fine_quarter(qr, qc):
        rows, cols = pl.ds(16 * qr, 16), pl.ds(2 * qc, 2)
        x = fv[rows, cols].astype(F32).reshape(256, 512)
        mx = mo[rows, cols].astype(F32).reshape(256, 512).astype(BF)
        att = (x + dot(mx, wproj[...])).astype(BF).astype(F32)
        n = norm(att).astype(BF)
        acc = att
        for s in range(4):
            cut = slice(512 * s, 512 * s + 512)
            hid = jax.nn.gelu(dot(n, wup[:, cut])).astype(BF)
            acc = acc + dot(hid, wdown[cut, :])
        out32 = acc.astype(BF).astype(F32)
        fo[rows, cols] = out32.reshape(16, 2, 8, 512).astype(BF)
        for t in range(4):
            fs[t] = out32[:, 128 * t : 128 * t + 128]
        for i in range(4):
            joined = jnp.concatenate(
                [
                    jnp.concatenate(
                        [
                            fs[t, pl.ds(64 * i + 32 * r + 16 * (p % 2) + p // 2, 8, stride=2), :]
                            for p in range(4)
                            for t in range(4)
                        ],
                        axis=1,
                    )
                    for r in range(2)
                ],
                axis=0,
            )
            at = pl.multiple_of(64 * (2 * qr + qc) + 16 * i, 16)
            jn[pl.ds(at, 16), :] = norm(joined).astype(BF)

    def merge(first, count):
        @pl.loop(0, 4)
        def _(s):
            cut = pl.ds(pl.multiple_of(256 * s, 256), 256)
            m = dot(jn[64 * first : 64 * (first + count), :], wmerge[:, cut])
            mg[first : first + count, :, :, cut] = m.reshape(count, 8, 8, 256).astype(BF)

    fine_quarter(1, 1)
    b[0].wait_recv()
    b[2].wait_recv()
    fine_quarter(1, 0)
    for at in (1, 3, 4):
        b[at].wait_recv()
    fine_quarter(0, 1)
    forward(3)
    fine_quarter(0, 0)
    merge(0, 3)
    a = [
        remote(mg.at[2], cr.at[1], cs, cq, 0, west),
        remote(mg.at[1], cr.at[2], cs, cq, 1, north),
        remote(mg.at[0], cr.at[3], cs, cq, 2, northwest),
    ]
    out_f = pltpu.make_async_copy(fo, fine_out, osem.at[0])
    out_f.start()
    forward(4)
    merge(3, 1)
    cr[0] = mg[3]
    pass_cross(4)
    for copy in a:
        copy.wait_recv()
    cxt[...] = norm(cr[...].astype(F32).reshape(256, 1024)).T.astype(BF)

    def project(gx, gc_):
        for r2 in range(2):
            w = wall[gx, gc_, pl.ds(4 * r2, 4)].reshape(512, 1024)
            got = dot(w, cxt[...]).astype(BF)
            for i in range(4):
                slot = ((z + OFFSETS[4 * r2 + i] + 8) % 8) * 4 + 2 * gx + gc_
                qkvt[pl.ds(pl.multiple_of(96 * slot, 32), 96), :] = got[128 * i : 128 * i + 96]
                pt[pl.ds(pl.multiple_of(32 * slot, 32), 32), :] = wall[
                    gx, gc_, 4 * r2 + i, 1, pl.ds(32, 32), :
                ]

    for k in range(5):
        ec[k].wait_recv()

    @pl.loop(0, 2)
    def _(g):
        project(xh, g)

    pass_twin(3)
    pass_twin(4)
    for k in range(5):
        gc[k].wait_recv()

    @pl.loop(0, 2)
    def _(g):
        project(1 - xh, g)

    c_lift = jnp.where(edge, F32(-1e30), F32(0.0))

    @pl.loop(0, 4)
    def _(j):
        bias = jnp.where(off_half, c_lift, F32(0.0))
        for i in range(2):
            at = pl.multiple_of(256 * j + 128 * i, 128)
            qt = (qkvt[pl.ds(at, 128), :].astype(F32) * 0.125).astype(BF)
            keys = qkvt[pl.ds(at + 1024, 128), :].astype(F32).T.astype(BF)
            vt = qkvt[pl.ds(at + 2048, 128), :]
            o = attend_pair(keys, qt, vt, bias).T
            cm[:, :, :, pl.ds(at, 128)] = o.reshape(4, 8, 8, 128).astype(BF)

    d = [
        remote(cm.at[1], cmo.at[2], ds_, dr, 0, east),
        remote(cm.at[2], cmo.at[1], ds_, dr, 1, south),
        remote(cm.at[3], cmo.at[0], ds_, dr, 2, southeast),
    ]
    cmo[3] = cm[0]
    for copy in d:
        copy.wait_recv()
    ot[...] = cmo[...].astype(F32).reshape(256, 1024).astype(BF)

    @pl.loop(0, 4)
    def _(s):
        at = pl.multiple_of(256 * s, 256)
        got = lax.dot_general(
            ot[...], pt[pl.ds(at, 256), :], (((1,), (1,)), ((), ())), preferred_element_type=F32
        )
        cut = pl.ds(at, 256)
        res = (mg[:, :, :, cut].astype(F32) + got.reshape(4, 8, 8, 256)).astype(BF)
        for q in range(4):
            co[pl.ds(8 * (q // 2), 8), q % 2, :, cut] = res[q]

    out_c = pltpu.make_async_copy(co, coarse_out, osem.at[1])
    out_c.start()
    for copy in sent:
        copy.wait_send()
    out_f.wait()
    out_c.wait()


def body(field, qkv_fine, proj_fine, up_fine, down_fine, merge_weight, qkv_coarse, proj_coarse):
    any_spec = pl.BlockSpec(memory_space=pl.ANY)
    dma = pltpu.SemaphoreType.DMA
    vm = pltpu.VMEM
    fine, coarse = pl.pallas_call(
        kernel,
        out_shape=(
            jax.ShapeDtypeStruct((32, 4, 8, 512), BF),
            jax.ShapeDtypeStruct((16, 2, 8, 1024), BF),
        ),
        in_specs=[any_spec] * 8,
        out_specs=(any_spec, any_spec),
        scratch_shapes=[
            vm((512, 1536), BF), vm((512, 512), BF), vm((512, 2048), BF), vm((2048, 512), BF),
            vm((2048, 1024), BF), vm((1024, 96), BF), vm((1024, 32), BF),
            vm((32, 4, 8, 512), BF), vm((32, 4, 8, 512), BF), vm((32, 4, 8, 512), BF),
            vm((32, 4, 8, 512), BF), vm((32, 4, 8, 512), BF),
            vm((4, 256, 128), F32), vm((256, 2048), BF),
            vm((4, 8, 8, 1024), BF), vm((4, 8, 8, 1024), BF), vm((1024, 256), BF),
            vm((2, 2, 8, 2, 64, 1024), BF), vm((3072, 256), BF), vm((256, 1024), BF),
            vm((4, 8, 8, 1024), BF), vm((4, 8, 8, 1024), BF), vm((16, 2, 8, 1024), BF),
            vm((1024, 1024), BF),
            dma((9,)), dma((2,)),
            dma((3,)), dma((3,)), dma((5,)), dma((5,)), dma((3,)), dma((3,)), dma((3,)), dma((3,)),
            dma((8,)), dma((8,)), dma((5,)), dma((5,)), dma((5,)), dma((5,)),
            dma((5,)), dma((5,)), dma((5,)), dma((5,)),
        ],
        compiler_params=pltpu.CompilerParams(
            collective_id=0, has_side_effects=True, vmem_limit_bytes=60 * 1024 * 1024
        ),
        name="encoder",
    )(field.reshape(32, 4, 8, 512), qkv_fine, proj_fine, up_fine, down_fine, merge_weight,
      qkv_coarse, proj_coarse)
    return fine.reshape(32, 32, 512), coarse.reshape(16, 16, 1024)


def solution(mesh):
    in_specs = (P("lat", "lon", None), P(), P(), P(), P(), P(), P(None, "lon"), P(None, "lon"))
    out_specs = (P("lat", "lon", None), P("lat", "lon", None))
    return jax.shard_map(body, mesh=mesh, in_specs=in_specs, out_specs=out_specs, check_vma=False)
```

```python
import jax
import jax.numpy as jnp
from jax import lax
from jax.experimental import pallas as pl
from jax.experimental.pallas import tpu as pltpu
from jax.sharding import PartitionSpec as P

MESH = pl.DeviceIdType.MESH
BF = jnp.bfloat16
F32 = jnp.float32
OFFSETS = (0, -1, 1, -2, 2, -3, 3, 4)
CHUNKS = ((0, 1), (1, 2), (3, 2), (5, 1), (6, 1), (7, 1))
LAST = len(CHUNKS)


def norm(v):
    center = v - jnp.mean(v, axis=-1, keepdims=True)
    spread = jnp.mean(center * center, axis=-1, keepdims=True)
    return center * lax.rsqrt(spread + 1e-05)


def dot(a, b):
    return jnp.dot(a, b, preferred_element_type=F32)


def attend_pair(keys, qt, vt, bias):
    zero = jnp.zeros((64, 256), BF)
    outs = []
    for half in range(2):
        part = qt[64 * half : 64 * half + 64]
        padded = jnp.concatenate([part, zero] if half == 0 else [zero, part], axis=0)
        scores = dot(keys, padded) + bias
        top = jnp.max(scores, axis=0, keepdims=True)
        p = jnp.exp(scores - top)
        total = jnp.sum(p, axis=0, keepdims=True)
        o = dot(vt[64 * half : 64 * half + 64], p.astype(BF))
        outs.append(o * (1.0 / total))
    return jnp.concatenate(outs, axis=0)


def kernel(
    field, wqkv_h, wproj_h, wup_h, wdown_h, wmerge_h, cqkv_h, cproj_h,
    fo, mg, ot, pt,
    wqkv, wproj, wup, wdown, wmerge,
    fv, xr, mr, mo, fs, jn, cr, cxt, wall, pall, qkvt, cm, cmo,
    lsem, hs, hr, bs, br, cs, cq, ds_, dr, zs, zr, xs, xq, ps, pr, es, er, gs, gr,
    zs2, zr2, xs2, xq2, ps2, pr2, es2, er2, gs2, gr2,
):
    lat = lax.axis_index("lat")
    lon = lax.axis_index("lon")
    xlo = lat // 4
    y = lat % 4
    z = lon // 4
    xh = (lon // 2) % 2
    c = lon % 2
    west = (lat, (lon + 31) % 32)
    east = (lat, (lon + 1) % 32)
    north = ((lat + 7) % 8, lon)
    south = ((lat + 1) % 8, lon)
    northwest = ((lat + 7) % 8, (lon + 31) % 32)
    southeast = ((lat + 1) % 8, (lon + 1) % 32)
    zup = (lat, ((z + 1) % 8) * 4 + xh * 2 + c)
    zdn = (lat, ((z + 7) % 8) * 4 + xh * 2 + c)
    cross = ((1 - xlo) * 4 + y, z * 4 + (1 - xh) * 2 + c)
    pair = ((1 - xlo) * 4 + y, lon)
    twin = (lat, z * 4 + xh * 2 + (1 - c))

    def local(src, dst, at):
        copy = pltpu.make_async_copy(src, dst, lsem.at[at])
        copy.start()
        return copy

    sent = []

    def remote(src, dst, ssem, rsem, at, device):
        copy = pltpu.make_async_remote_copy(
            src_ref=src, dst_ref=dst, send_sem=ssem.at[at], recv_sem=rsem.at[at],
            device_id=device, device_id_type=MESH,
        )
        copy.start()
        sent.append(copy)
        return copy

    own_x = local(field.at[pl.ds(8, 24), pl.ds(1, 3)], xr.at[pl.ds(0, 24), pl.ds(0, 3)], 0)
    own_q = local(cqkv_h, wall.at[xh, c, 0], 7)
    own_p = local(cproj_h, pall.at[xh, c, 0], 8)
    l_qkv = local(wqkv_h, wqkv, 1)
    own_f = local(field, fv, 2)
    l_proj = local(wproj_h, wproj, 3)
    l_up = local(wup_h, wup, 4)
    l_down = local(wdown_h, wdown, 5)
    l_merge = local(wmerge_h, wmerge, 6)

    barrier = pltpu.get_barrier_semaphore()
    peers = (west, east, north, south, northwest, southeast, zup, zdn, cross, pair, twin)
    for peer in peers:
        pl.semaphore_signal(barrier, inc=1, device_id=peer, device_id_type=MESH)
    pl.semaphore_wait(barrier, len(peers))

    h = [
        remote(field.at[pl.ds(8, 24), 0], xr.at[pl.ds(0, 24), 3], hs, hr, 0, west),
        remote(field.at[pl.ds(0, 8), pl.ds(1, 3)], xr.at[pl.ds(24, 8), pl.ds(0, 3)], hs, hr, 1, north),
        remote(field.at[pl.ds(0, 8), 0], xr.at[pl.ds(24, 8), 3], hs, hr, 2, northwest),
    ]

    class Gather:
        def __init__(self, wall, zs, zr, xs, xq, ps, pr, es, er, gs, gr):
            self.wall = wall
            self.sems = dict(z=(zs, zr), x=(xs, xq), p=(ps, pr), e=(es, er), g=(gs, gr))
            self.made = dict(z={}, x={}, p={}, e={}, g={})

        def send(self, kind, at, src, dst, device):
            self.made[kind][at] = remote(src, dst, *self.sems[kind], at, device)

        def arrive(self, kind, *ats):
            for at in ats:
                self.made[kind][at].wait_recv()

        def send_z(self, step):
            own = self.wall.at[xh, c]
            if step == 0:
                self.send("z", 0, own.at[0], own.at[1], zup)
                self.send("z", 1, own.at[0], own.at[2], zdn)
            elif step < 3:
                a = 2 * step
                self.send("z", a, own.at[a - 1], own.at[a + 1], zup)
                self.send("z", a + 1, own.at[a], own.at[a + 2], zdn)
            else:
                self.send("z", 6, own.at[5, 0], own.at[7, 0], zup)
                self.send("z", 7, own.at[6, 1], own.at[7, 1], zdn)

        def own_chunk(self, k):
            at, n = CHUNKS[k]
            half = self.wall.at[xh, c, pl.ds(at, n), xlo]
            full = self.wall.at[xh, c, pl.ds(at, n)]
            self.send("x", k, half, half, cross)
            self.send("e", k, full, full, twin)

        def pass_cross(self, *ks):
            for k in ks:
                at, n = CHUNKS[k]
                self.arrive("x", k)
                ref = self.wall.at[1 - xh, c, pl.ds(at, n), 1 - xlo]
                self.send("p", k, ref, ref, pair)

        def pass_twin(self, *ks):
            for k in ks:
                at, n = CHUNKS[k]
                self.arrive("p", k)
                ref = self.wall.at[1 - xh, c, pl.ds(at, n)]
                self.send("g", k, ref, ref, twin)

        def start(self):
            self.send_z(0)
            self.own_chunk(0)

        def forward(self, k):
            self.arrive("z", 2 * k - 2, 2 * k - 1)
            if k < 4:
                self.send_z(k)
            for chunk in ((1,), (2,), (3, 4), (5,))[k - 1]:
                self.own_chunk(chunk)
            if k < 4:
                self.pass_cross(k - 1)
            if k >= 2:
                self.pass_twin(k - 2)

    main = Gather(wall, zs, zr, xs, xq, ps, pr, es, er, gs, gr)
    tail = Gather(pall, zs2, zr2, xs2, xq2, ps2, pr2, es2, er2, gs2, gr2)

    own_q.wait()
    own_p.wait()
    main.start()

    off_half = (lax.broadcasted_iota(jnp.int32, (256, 256), 0) >= 128) != (
        lax.broadcasted_iota(jnp.int32, (256, 256), 1) >= 128
    )
    edge = lat == 7

    def fine_window(wr, wc):
        lift = jnp.where(jnp.logical_and(edge, wr == 1), F32(-1e30), F32(0.0))
        bias = jnp.where(off_half, lift, F32(0.0))
        x = xr[pl.ds(16 * wr, 16), pl.ds(2 * wc, 2)].astype(F32).reshape(256, 512)
        xn = norm(x).astype(BF)
        q = (dot(xn, wqkv[:, 0:512])).astype(BF).astype(F32) * 0.125
        keys = dot(xn, wqkv[:, 512:1024]).astype(BF)
        v = dot(xn, wqkv[:, 1024:1536])
        qt = q.T.astype(BF)
        vt = v.T.astype(BF)
        outs = []
        for j in range(4):
            cut = slice(128 * j, 128 * j + 128)
            outs.append(attend_pair(keys[:, cut], qt[cut], vt[cut], bias).T)
        res = jnp.concatenate(outs, axis=1)
        mr[pl.ds(16 * wr, 16), pl.ds(2 * wc, 2)] = res.reshape(16, 2, 8, 512).astype(BF)

    own_x.wait()
    l_qkv.wait()
    fine_window(0, 0)
    h[0].wait_recv()
    fine_window(0, 1)
    b = [remote(mr.at[pl.ds(0, 16), 3], mo.at[pl.ds(8, 16), 0], bs, br, 0, east)]
    h[1].wait_recv()
    h[2].wait_recv()
    main.forward(1)
    fine_window(1, 0)
    b.append(remote(mr.at[pl.ds(24, 8), pl.ds(0, 2)], mo.at[pl.ds(0, 8), pl.ds(1, 2)], bs, br, 1, south))
    fine_window(1, 1)
    b.append(remote(mr.at[pl.ds(16, 8), 3], mo.at[pl.ds(24, 8), 0], bs, br, 2, east))
    b.append(remote(mr.at[pl.ds(24, 8), 2], mo.at[pl.ds(0, 8), 3], bs, br, 3, south))
    b.append(remote(mr.at[pl.ds(24, 8), 3], mo.at[pl.ds(0, 8), 0], bs, br, 4, southeast))
    main.forward(2)
    tail.start()
    mo[pl.ds(8, 24), pl.ds(1, 3)] = mr[pl.ds(0, 24), pl.ds(0, 3)]
    for copy in (own_f, l_proj, l_up, l_down, l_merge):
        copy.wait()

    def fine_quarter(qr, qc):
        rows, cols = pl.ds(16 * qr, 16), pl.ds(2 * qc, 2)
        x = fv[rows, cols].astype(F32).reshape(256, 512)
        mx = mo[rows, cols].astype(F32).reshape(256, 512).astype(BF)
        att = (x + dot(mx, wproj[...])).astype(BF).astype(F32)
        n = norm(att).astype(BF)
        acc = att
        for s in range(4):
            cut = slice(512 * s, 512 * s + 512)
            hid = jax.nn.gelu(dot(n, wup[:, cut])).astype(BF)
            acc = acc + dot(hid, wdown[cut, :])
        out32 = acc.astype(BF).astype(F32)
        fo[rows, cols] = out32.reshape(16, 2, 8, 512).astype(BF)
        for t in range(4):
            fs[t] = out32[:, 128 * t : 128 * t + 128]
        for i in range(4):
            joined = jnp.concatenate(
                [
                    jnp.concatenate(
                        [
                            fs[t, pl.ds(64 * i + 32 * r + 16 * (p % 2) + p // 2, 8, stride=2), :]
                            for p in range(4)
                            for t in range(4)
                        ],
                        axis=1,
                    )
                    for r in range(2)
                ],
                axis=0,
            )
            at = pl.multiple_of(64 * (2 * qr + qc) + 16 * i, 16)
            jn[pl.ds(at, 16), :] = norm(joined).astype(BF)

    def merge(first, count):
        @pl.loop(0, 4)
        def _(s):
            cut = pl.ds(pl.multiple_of(256 * s, 256), 256)
            m = dot(jn[64 * first : 64 * (first + count), :], wmerge[:, cut])
            mg[first : first + count, :, :, cut] = m.reshape(count, 8, 8, 256).astype(BF)

    fine_quarter(1, 1)
    b[0].wait_recv()
    b[2].wait_recv()
    fine_quarter(1, 0)
    for at in (1, 3, 4):
        b[at].wait_recv()
    fine_quarter(0, 1)
    main.forward(3)
    tail.forward(1)
    fine_quarter(0, 0)
    merge(0, 3)
    a = [
        remote(mg.at[2], cr.at[1], cs, cq, 0, west),
        remote(mg.at[1], cr.at[2], cs, cq, 1, north),
        remote(mg.at[0], cr.at[3], cs, cq, 2, northwest),
    ]
    main.forward(4)
    main.pass_cross(3)
    tail.forward(2)
    merge(3, 1)
    cr[0] = mg[3]
    main.pass_cross(4, 5)
    for copy in a:
        copy.wait_recv()
    main.pass_twin(3)
    tail.forward(3)
    cxt[...] = norm(cr[...].astype(F32).reshape(256, 1024)).T.astype(BF)

    def project(gx, gc_):
        for r2 in range(2):
            w = wall[gx, gc_, pl.ds(4 * r2, 4)].reshape(384, 1024)
            got = dot(w, cxt[...]).astype(BF)
            for i in range(4):
                slot = ((z + OFFSETS[4 * r2 + i] + 8) % 8) * 4 + 2 * gx + gc_
                qkvt[pl.ds(pl.multiple_of(96 * slot, 32), 96), :] = got[96 * i : 96 * i + 96]

    main.arrive("e", *range(LAST))

    @pl.loop(0, 2)
    def _(g):
        project(xh, g)

    main.pass_twin(4, 5)
    tail.forward(4)
    project(1 - xh, c)
    main.arrive("g", *range(LAST))
    project(1 - xh, 1 - c)
    tail.pass_cross(3, 4, 5)

    c_lift = jnp.where(edge, F32(-1e30), F32(0.0))

    def coarse_heads(first):
        @pl.loop(first, first + 2)
        def _(j):
            bias = jnp.where(off_half, c_lift, F32(0.0))
            for i in range(2):
                at = pl.multiple_of(256 * j + 128 * i, 128)
                qt = (qkvt[pl.ds(at, 128), :].astype(F32) * 0.125).astype(BF)
                keys = qkvt[pl.ds(at + 1024, 128), :].astype(F32).T.astype(BF)
                vt = qkvt[pl.ds(at + 2048, 128), :]
                o = attend_pair(keys, qt, vt, bias).T
                cm[:, :, :, pl.ds(at, 128)] = o.reshape(4, 8, 8, 128).astype(BF)

    d = []
    for part in range(2):
        coarse_heads(2 * part)
        if part == 0:
            tail.pass_twin(3, 4, 5)
        cut = pl.ds(512 * part, 512)
        for i, (src, dst, device) in enumerate(((1, 2, east), (2, 1, south), (3, 0, southeast))):
            d.append(
                remote(cm.at[src, :, :, cut], cmo.at[dst, :, :, cut], ds_, dr, 3 * part + i, device)
            )
    cmo[3] = cm[0]
    tail.arrive("e", *range(LAST))
    tail.arrive("g", *range(LAST))

    @pl.loop(0, 4)
    def _(g):
        for r in range(8):
            slot = ((z + OFFSETS[r] + 8) % 8) * 4 + g
            pt[pl.ds(pl.multiple_of(32 * slot, 32), 32), :] = pall[g // 2, g % 2, r].reshape(32, 1024)

    for copy in d:
        copy.wait_recv()
    ot[...] = cmo[...].astype(F32).reshape(256, 1024).astype(BF)

    for copy in sent:
        copy.wait_send()


def finish(fo, mg, ot, pt, fine_out, coarse_out, co, osem):
    out_f = pltpu.make_async_copy(fo, fine_out, osem.at[0])
    out_f.start()

    @pl.loop(0, 4)
    def _(s):
        at = pl.multiple_of(256 * s, 256)
        got = lax.dot_general(
            ot[...], pt[pl.ds(at, 256), :], (((1,), (1,)), ((), ())), preferred_element_type=F32
        )
        cut = pl.ds(at, 256)
        res = (mg[:, :, :, cut].astype(F32) + got.reshape(4, 8, 8, 256)).astype(BF)
        for q in range(4):
            co[pl.ds(8 * (q // 2), 8), q % 2, :, cut] = res[q]

    out_c = pltpu.make_async_copy(co, coarse_out, osem.at[1])
    out_c.start()
    out_f.wait()
    out_c.wait()


def body(field, qkv_fine, proj_fine, up_fine, down_fine, merge_weight, qkv_coarse, proj_coarse):
    any_spec = pl.BlockSpec(memory_space=pltpu.HBM)
    dma = pltpu.SemaphoreType.DMA
    vm = pltpu.VMEM
    in_vmem = pl.BlockSpec(memory_space=pltpu.VMEM)
    held = pl.pallas_call(
        kernel,
        out_shape=(
            pltpu.VMEM((32, 4, 8, 512), BF),
            pltpu.VMEM((4, 8, 8, 1024), BF),
            pltpu.VMEM((256, 1024), BF),
            pltpu.VMEM((1024, 1024), BF),
        ),
        in_specs=[any_spec] * 8,
        out_specs=(in_vmem,) * 4,
        scratch_shapes=[
            vm((512, 1536), BF), vm((512, 512), BF), vm((512, 2048), BF), vm((2048, 512), BF),
            vm((2048, 1024), BF),
            vm((32, 4, 8, 512), BF), vm((32, 4, 8, 512), BF), vm((32, 4, 8, 512), BF),
            vm((32, 4, 8, 512), BF),
            vm((4, 256, 128), F32), vm((256, 2048), BF),
            vm((4, 8, 8, 1024), BF), vm((1024, 256), BF),
            vm((2, 2, 8, 2, 48, 1024), BF), vm((2, 2, 8, 2, 16, 1024), BF), vm((3072, 256), BF),
            vm((4, 8, 8, 1024), BF), vm((4, 8, 8, 1024), BF),
            dma((9,)),
            *[dma((n,)) for n in (3, 3, 5, 5, 3, 3, 6, 6)],
            *[dma((n,)) for n in (8, 8, 6, 6, 6, 6, 6, 6, 6, 6)],
            *[dma((n,)) for n in (8, 8, 6, 6, 6, 6, 6, 6, 6, 6)],
        ],
        compiler_params=pltpu.CompilerParams(
            collective_id=0, has_side_effects=True, vmem_limit_bytes=59 * 1024 * 1024
        ),
        name="encoder",
    )(field.reshape(32, 4, 8, 512), qkv_fine, proj_fine, up_fine, down_fine, merge_weight,
      qkv_coarse.T.reshape(2, 48, 1024), proj_coarse.T.reshape(2, 16, 1024))
    fine, coarse = pl.pallas_call(
        finish,
        out_shape=(
            jax.ShapeDtypeStruct((32, 4, 8, 512), BF),
            jax.ShapeDtypeStruct((16, 2, 8, 1024), BF),
        ),
        in_specs=[in_vmem] * 4,
        out_specs=(any_spec, any_spec),
        scratch_shapes=[vm((16, 2, 8, 1024), BF), dma((2,))],
        compiler_params=pltpu.CompilerParams(vmem_limit_bytes=8 * 1024 * 1024),
        name="finish",
    )(*held)
    return fine.reshape(32, 32, 512), coarse.reshape(16, 16, 1024)


def solution(mesh):
    in_specs = (P("lat", "lon", None), P(), P(), P(), P(), P(), P(None, "lon"), P(None, "lon"))
    out_specs = (P("lat", "lon", None), P("lat", "lon", None))
    return jax.shard_map(body, mesh=mesh, in_specs=in_specs, out_specs=out_specs, check_vma=False)
```

```python
import jax
import jax.numpy as jnp
from jax import lax
from jax.experimental import pallas as pl
from jax.experimental.pallas import tpu as pltpu
from jax.sharding import PartitionSpec as P

MESH = pl.DeviceIdType.MESH
BF = jnp.bfloat16
F32 = jnp.float32
SCALE = 0.125 * 1.4426950408889634
OFFSETS = (0, -1, 1, -2, 2, -3, 3, 4)
CHUNKS = ((0, 1), (1, 2), (3, 2), (5, 1), (6, 1), (7, 1))
LAST = len(CHUNKS)


def norm(v):
    center = v - jnp.mean(v, axis=-1, keepdims=True)
    spread = jnp.mean(center * center, axis=-1, keepdims=True)
    return center * lax.rsqrt(spread + 1e-05)


def dot(a, b):
    return jnp.dot(a, b, preferred_element_type=F32)


def attend_pair(keys, qt, vt, bias):
    zero = jnp.zeros((64, 256), BF)
    outs = []
    for half in range(2):
        part = qt[64 * half : 64 * half + 64]
        padded = jnp.concatenate([part, zero] if half == 0 else [zero, part], axis=0)
        scores = dot(keys, padded)
        if bias is not None:
            scores = scores + bias
        top = jnp.max(scores, axis=0, keepdims=True)
        p = jnp.exp2(scores - top)
        total = jnp.sum(p, axis=0, keepdims=True)
        o = dot(vt[64 * half : 64 * half + 64], p.astype(BF))
        outs.append(o * (1.0 / total))
    return jnp.concatenate(outs, axis=0)


def kernel(
    field, wqkv_h, wproj_h, wup_h, wdown_h, wmerge_h, cqkv_h, cproj_h,
    fo, mg, ot, pt,
    wqkv, wproj, wup, wdown, wmerge,
    fv, xr, mr, mo, fs, jn, cr, cxt, wall, pall, qkvt, cm, cmo,
    lsem, hs, hr, bs, br, cs, cq, ds_, dr, zs, zr, xs, xq, ps, pr, es, er, gs, gr,
    zs2, zr2, xs2, xq2, ps2, pr2, es2, er2, gs2, gr2,
):
    lat = lax.axis_index("lat")
    lon = lax.axis_index("lon")
    xlo = lat // 4
    y = lat % 4
    z = lon // 4
    xh = (lon // 2) % 2
    c = lon % 2
    west = (lat, (lon + 31) % 32)
    east = (lat, (lon + 1) % 32)
    north = ((lat + 7) % 8, lon)
    south = ((lat + 1) % 8, lon)
    northwest = ((lat + 7) % 8, (lon + 31) % 32)
    southeast = ((lat + 1) % 8, (lon + 1) % 32)
    zup = (lat, ((z + 1) % 8) * 4 + xh * 2 + c)
    zdn = (lat, ((z + 7) % 8) * 4 + xh * 2 + c)
    cross = ((1 - xlo) * 4 + y, z * 4 + (1 - xh) * 2 + c)
    pair = ((1 - xlo) * 4 + y, lon)
    twin = (lat, z * 4 + xh * 2 + (1 - c))

    def local(src, dst, at):
        copy = pltpu.make_async_copy(src, dst, lsem.at[at])
        copy.start()
        return copy

    sent = []

    def remote(src, dst, ssem, rsem, at, device):
        copy = pltpu.make_async_remote_copy(
            src_ref=src, dst_ref=dst, send_sem=ssem.at[at], recv_sem=rsem.at[at],
            device_id=device, device_id_type=MESH,
        )
        copy.start()
        sent.append(copy)
        return copy

    own_x = local(field.at[pl.ds(8, 24), pl.ds(1, 3)], xr.at[pl.ds(0, 24), pl.ds(0, 3)], 0)
    own_q = local(cqkv_h, wall.at[xh, c, 0], 7)
    own_p = local(cproj_h, pall.at[xh, c, 0], 8)
    l_qkv = local(wqkv_h, wqkv, 1)
    own_f = local(field, fv, 2)
    l_proj = local(wproj_h, wproj, 3)
    l_up = local(wup_h, wup, 4)
    l_down = local(wdown_h, wdown, 5)
    l_merge = local(wmerge_h, wmerge, 6)

    barrier = pltpu.get_barrier_semaphore()
    peers = (west, east, north, south, northwest, southeast, zup, zdn, cross, pair, twin)
    for peer in peers:
        pl.semaphore_signal(barrier, inc=1, device_id=peer, device_id_type=MESH)
    pl.semaphore_wait(barrier, len(peers))

    h = [
        remote(field.at[pl.ds(8, 24), 0], xr.at[pl.ds(0, 24), 3], hs, hr, 0, west),
        remote(field.at[pl.ds(0, 8), pl.ds(1, 3)], xr.at[pl.ds(24, 8), pl.ds(0, 3)], hs, hr, 1, north),
        remote(field.at[pl.ds(0, 8), 0], xr.at[pl.ds(24, 8), 3], hs, hr, 2, northwest),
    ]

    class Gather:
        def __init__(self, wall, zs, zr, xs, xq, ps, pr, es, er, gs, gr):
            self.wall = wall
            self.sems = dict(z=(zs, zr), x=(xs, xq), p=(ps, pr), e=(es, er), g=(gs, gr))
            self.made = dict(z={}, x={}, p={}, e={}, g={})

        def send(self, kind, at, src, dst, device):
            self.made[kind][at] = remote(src, dst, *self.sems[kind], at, device)

        def arrive(self, kind, *ats):
            for at in ats:
                self.made[kind][at].wait_recv()

        def send_z(self, step):
            own = self.wall.at[xh, c]
            if step == 0:
                self.send("z", 0, own.at[0], own.at[1], zup)
                self.send("z", 1, own.at[0], own.at[2], zdn)
            elif step < 3:
                a = 2 * step
                self.send("z", a, own.at[a - 1], own.at[a + 1], zup)
                self.send("z", a + 1, own.at[a], own.at[a + 2], zdn)
            else:
                self.send("z", 6, own.at[5, 0], own.at[7, 0], zup)
                self.send("z", 7, own.at[6, 1], own.at[7, 1], zdn)

        def own_chunk(self, k):
            at, n = CHUNKS[k]
            half = self.wall.at[xh, c, pl.ds(at, n), xlo]
            full = self.wall.at[xh, c, pl.ds(at, n)]
            self.send("x", k, half, half, cross)
            self.send("e", k, full, full, twin)

        def pass_cross(self, *ks):
            for k in ks:
                at, n = CHUNKS[k]
                self.arrive("x", k)
                ref = self.wall.at[1 - xh, c, pl.ds(at, n), 1 - xlo]
                self.send("p", k, ref, ref, pair)

        def pass_twin(self, *ks):
            for k in ks:
                at, n = CHUNKS[k]
                self.arrive("p", k)
                ref = self.wall.at[1 - xh, c, pl.ds(at, n)]
                self.send("g", k, ref, ref, twin)

        def start(self):
            self.send_z(0)
            self.own_chunk(0)

        def forward(self, k):
            self.arrive("z", 2 * k - 2, 2 * k - 1)
            if k < 4:
                self.send_z(k)
            for chunk in ((1,), (2,), (3, 4), (5,))[k - 1]:
                self.own_chunk(chunk)
            if k < 4:
                self.pass_cross(k - 1)
            if 2 <= k < 4:
                self.pass_twin(k - 2)

    main = Gather(wall, zs, zr, xs, xq, ps, pr, es, er, gs, gr)
    tail = Gather(pall, zs2, zr2, xs2, xq2, ps2, pr2, es2, er2, gs2, gr2)

    own_q.wait()
    own_p.wait()
    main.start()

    off_half = (lax.broadcasted_iota(jnp.int32, (256, 256), 0) >= 128) != (
        lax.broadcasted_iota(jnp.int32, (256, 256), 1) >= 128
    )
    lift = jnp.where(lat == 7, F32(-1e30), F32(0.0))

    def fine_window(wr, wc):
        bias = jnp.where(off_half, lift, F32(0.0)) if wr == 1 else None
        x = xr[pl.ds(16 * wr, 16), pl.ds(2 * wc, 2)].astype(F32).reshape(256, 512)
        xn = norm(x).astype(BF)
        q = dot(xn, wqkv[:, 0:512]) * SCALE
        keys = dot(xn, wqkv[:, 512:1024]).astype(BF)
        v = dot(xn, wqkv[:, 1024:1536])
        qt = q.T.astype(BF)
        vt = v.T.astype(BF)
        outs = []
        for j in range(4):
            cut = slice(128 * j, 128 * j + 128)
            outs.append(attend_pair(keys[:, cut], qt[cut], vt[cut], bias).T)
        res = jnp.concatenate(outs, axis=1)
        mr[pl.ds(16 * wr, 16), pl.ds(2 * wc, 2)] = res.reshape(16, 2, 8, 512).astype(BF)

    own_x.wait()
    l_qkv.wait()
    fine_window(0, 0)
    h[0].wait_recv()
    fine_window(0, 1)
    b = [remote(mr.at[pl.ds(0, 16), 3], mo.at[pl.ds(8, 16), 0], bs, br, 0, east)]
    h[1].wait_recv()
    h[2].wait_recv()
    main.forward(1)
    fine_window(1, 0)
    b.append(remote(mr.at[pl.ds(24, 8), pl.ds(0, 2)], mo.at[pl.ds(0, 8), pl.ds(1, 2)], bs, br, 1, south))
    fine_window(1, 1)
    b.append(remote(mr.at[pl.ds(16, 8), 3], mo.at[pl.ds(24, 8), 0], bs, br, 2, east))
    b.append(remote(mr.at[pl.ds(24, 8), 2], mo.at[pl.ds(0, 8), 3], bs, br, 3, south))
    b.append(remote(mr.at[pl.ds(24, 8), 3], mo.at[pl.ds(0, 8), 0], bs, br, 4, southeast))
    main.forward(2)
    mo[pl.ds(8, 24), pl.ds(1, 3)] = mr[pl.ds(0, 24), pl.ds(0, 3)]
    for copy in (own_f, l_proj, l_up, l_down, l_merge):
        copy.wait()

    def fine_quarter(qr, qc):
        rows, cols = pl.ds(16 * qr, 16), pl.ds(2 * qc, 2)
        x = fv[rows, cols].astype(F32).reshape(256, 512)
        mx = mo[rows, cols].astype(F32).reshape(256, 512).astype(BF)
        att = (x + dot(mx, wproj[...])).astype(BF).astype(F32)
        n = norm(att).astype(BF)
        acc = att
        for s in range(4):
            cut = slice(512 * s, 512 * s + 512)
            hid = jax.nn.gelu(dot(n, wup[:, cut])).astype(BF)
            acc = acc + dot(hid, wdown[cut, :])
        out32 = acc.astype(BF).astype(F32)
        fo[rows, cols] = out32.reshape(16, 2, 8, 512).astype(BF)
        for t in range(4):
            fs[t] = out32[:, 128 * t : 128 * t + 128]
        for i in range(4):
            joined = jnp.concatenate(
                [
                    jnp.concatenate(
                        [
                            fs[t, pl.ds(64 * i + 32 * r + 16 * (p % 2) + p // 2, 8, stride=2), :]
                            for p in range(4)
                            for t in range(4)
                        ],
                        axis=1,
                    )
                    for r in range(2)
                ],
                axis=0,
            )
            at = pl.multiple_of(64 * (2 * qr + qc) + 16 * i, 16)
            jn[pl.ds(at, 16), :] = norm(joined).astype(BF)

    def merge(first, count):
        @pl.loop(0, 4)
        def _(s):
            cut = pl.ds(pl.multiple_of(256 * s, 256), 256)
            m = dot(jn[64 * first : 64 * (first + count), :], wmerge[:, cut])
            mg[first : first + count, :, :, cut] = m.reshape(count, 8, 8, 256).astype(BF)

    fine_quarter(1, 1)
    b[0].wait_recv()
    b[2].wait_recv()
    fine_quarter(1, 0)
    main.forward(3)
    tail.start()
    for at in (1, 3, 4):
        b[at].wait_recv()
    fine_quarter(0, 1)
    fine_quarter(0, 0)
    main.forward(4)
    tail.forward(1)
    merge(0, 3)
    a = [
        remote(mg.at[2], cr.at[1], cs, cq, 0, west),
        remote(mg.at[1], cr.at[2], cs, cq, 1, north),
        remote(mg.at[0], cr.at[3], cs, cq, 2, northwest),
    ]
    main.pass_twin(2)
    main.pass_cross(3)
    tail.forward(2)
    merge(3, 1)
    cr[0] = mg[3]
    main.pass_cross(4, 5)
    for copy in a:
        copy.wait_recv()
    main.pass_twin(3)
    cxt[...] = norm(cr[...].astype(F32).reshape(256, 1024)).T.astype(BF)
    tail.forward(3)

    def project(gx, gc_):
        for r2 in range(2):
            w = wall[gx, gc_, pl.ds(4 * r2, 4)].reshape(384, 1024)
            got = dot(w, cxt[...]).astype(BF)
            for i in range(4):
                slot = ((z + OFFSETS[4 * r2 + i] + 8) % 8) * 4 + 2 * gx + gc_
                qkvt[pl.ds(pl.multiple_of(96 * slot, 32), 96), :] = got[96 * i : 96 * i + 96]

    main.arrive("e", *range(LAST))

    @pl.loop(0, 2)
    def _(g):
        project(xh, g)

    main.pass_twin(4, 5)
    tail.forward(4)
    tail.pass_twin(2)
    project(1 - xh, c)
    main.arrive("g", *range(LAST))
    project(1 - xh, 1 - c)

    c_bias = jnp.where(off_half, lift, F32(0.0))
    d = []
    for part in range(4):
        for i in range(2):
            at = 256 * part + 128 * i
            qt = (qkvt[at : at + 128, :].astype(F32) * SCALE).astype(BF)
            keys = qkvt[at + 1024 : at + 1152, :].astype(F32).T.astype(BF)
            vt = qkvt[at + 2048 : at + 2176, :]
            o = attend_pair(keys, qt, vt, c_bias).T
            cm[:, :, :, at : at + 128] = o.reshape(4, 8, 8, 128).astype(BF)
        cut = pl.ds(256 * part, 256)
        for i, (src, dst, device) in enumerate(((1, 2, east), (2, 1, south), (3, 0, southeast))):
            d.append(
                remote(cm.at[src, :, :, cut], cmo.at[dst, :, :, cut], ds_, dr, 3 * part + i, device)
            )
        if part == 0:
            tail.pass_cross(3, 4, 5)
        if part == 3:
            tail.pass_twin(3, 4, 5)
    cmo[3] = cm[0]
    tail.arrive("e", *range(LAST))
    tail.arrive("g", *range(LAST))

    @pl.loop(0, 4)
    def _(g):
        for r in range(8):
            slot = ((z + OFFSETS[r] + 8) % 8) * 4 + g
            pt[pl.ds(pl.multiple_of(32 * slot, 32), 32), :] = pall[g // 2, g % 2, r].reshape(32, 1024)

    for copy in d:
        copy.wait_recv()
    ot[...] = cmo[...].astype(F32).reshape(256, 1024).astype(BF)

    for copy in sent:
        copy.wait_send()


def finish(fo, mg, ot, pt, fine_out, coarse_out, co, osem):
    out_f = pltpu.make_async_copy(fo, fine_out, osem.at[0])
    out_f.start()

    @pl.loop(0, 4)
    def _(s):
        at = pl.multiple_of(256 * s, 256)
        got = lax.dot_general(
            ot[...], pt[pl.ds(at, 256), :], (((1,), (1,)), ((), ())), preferred_element_type=F32
        )
        cut = pl.ds(at, 256)
        res = (mg[:, :, :, cut].astype(F32) + got.reshape(4, 8, 8, 256)).astype(BF)
        for q in range(4):
            co[pl.ds(8 * (q // 2), 8), q % 2, :, cut] = res[q]

    out_c = pltpu.make_async_copy(co, coarse_out, osem.at[1])
    out_c.start()
    out_f.wait()
    out_c.wait()


def body(field, qkv_fine, proj_fine, up_fine, down_fine, merge_weight, qkv_coarse, proj_coarse):
    any_spec = pl.BlockSpec(memory_space=pltpu.HBM)
    dma = pltpu.SemaphoreType.DMA
    vm = pltpu.VMEM
    in_vmem = pl.BlockSpec(memory_space=pltpu.VMEM)
    held = pl.pallas_call(
        kernel,
        out_shape=(
            pltpu.VMEM((32, 4, 8, 512), BF),
            pltpu.VMEM((4, 8, 8, 1024), BF),
            pltpu.VMEM((256, 1024), BF),
            pltpu.VMEM((1024, 1024), BF),
        ),
        in_specs=[any_spec] * 8,
        out_specs=(in_vmem,) * 4,
        scratch_shapes=[
            vm((512, 1536), BF), vm((512, 512), BF), vm((512, 2048), BF), vm((2048, 512), BF),
            vm((2048, 1024), BF),
            vm((32, 4, 8, 512), BF), vm((32, 4, 8, 512), BF), vm((32, 4, 8, 512), BF),
            vm((32, 4, 8, 512), BF),
            vm((4, 256, 128), F32), vm((256, 2048), BF),
            vm((4, 8, 8, 1024), BF), vm((1024, 256), BF),
            vm((2, 2, 8, 2, 48, 1024), BF), vm((2, 2, 8, 2, 16, 1024), BF), vm((3072, 256), BF),
            vm((4, 8, 8, 1024), BF), vm((4, 8, 8, 1024), BF),
            dma((9,)),
            *[dma((n,)) for n in (3, 3, 5, 5, 3, 3, 12, 12)],
            *[dma((n,)) for n in (8, 8, 6, 6, 6, 6, 6, 6, 6, 6)],
            *[dma((n,)) for n in (8, 8, 6, 6, 6, 6, 6, 6, 6, 6)],
        ],
        compiler_params=pltpu.CompilerParams(
            collective_id=0, has_side_effects=True, vmem_limit_bytes=59 * 1024 * 1024
        ),
        name="encoder",
    )(field.reshape(32, 4, 8, 512), qkv_fine, proj_fine, up_fine, down_fine, merge_weight,
      qkv_coarse.T.reshape(2, 48, 1024), proj_coarse.T.reshape(2, 16, 1024))
    fine, coarse = pl.pallas_call(
        finish,
        out_shape=(
            jax.ShapeDtypeStruct((32, 4, 8, 512), BF),
            jax.ShapeDtypeStruct((16, 2, 8, 1024), BF),
        ),
        in_specs=[in_vmem] * 4,
        out_specs=(any_spec, any_spec),
        scratch_shapes=[vm((16, 2, 8, 1024), BF), dma((2,))],
        compiler_params=pltpu.CompilerParams(vmem_limit_bytes=8 * 1024 * 1024),
        name="finish",
    )(*held)
    return fine.reshape(32, 32, 512), coarse.reshape(16, 16, 1024)


def solution(mesh):
    in_specs = (P("lat", "lon", None), P(), P(), P(), P(), P(), P(None, "lon"), P(None, "lon"))
    out_specs = (P("lat", "lon", None), P("lat", "lon", None))
    return jax.shard_map(body, mesh=mesh, in_specs=in_specs, out_specs=out_specs, check_vma=False)
```
